32 devices in a mesh: obs: 4 (over z), face: 8 (over y, x, core).
Axes of the slice: x: 2, y: 2, z: 4, core: 2. Of those that a mesh axis runs over, the one named last changes fastest.
Arguments:
- density: float32 [34, 8192], P(None, ('obs', 'face')), may hold values from 0.6 to 1.4
- velocity: float32 [3, 34, 8192], P(None, None, ('obs', 'face')), may hold values from -6 to 6
- pressure: float32 [34, 8192], P(None, ('obs', 'face')), may hold values from -6 to 6
- normal: float32 [3, 8192], P(None, ('obs', 'face')), may hold values from -1 to 1, as said below
- direction: float32 [32, 8, 3], P(('obs', 'face')), may hold values from -1 to 1, as said below
- weights: bfloat16 [32, 8, 768, 256], P(('obs', 'face')), may hold values from -0.21875 to 0.21875
- bin_index: int32 [32, 8], P(('obs', 'face')), may hold values from 0 to 7, as said below
- group_index: int32 [32, 8], P(('obs', 'face')), may hold values from 0 to 3
- item_count: int32 [32], P(('obs', 'face')), may hold values from 4 to 8, as said below
Outputs:
- signal: float32 [256, 1024], P('face', 'obs')
The draws below stay inside these ranges and needn't reach their ends.
Inputs may be any that keep to these rules, and one draw needn't show every extreme that they name: `bin_index`: no time block is named more than 2 times in one device's list; in every draw some device names a block 2 times among its live entries. `item_count`: some device has all 8 entries live. Each face's normal has unit length. Each entry's direction has unit length.
All inputs are finite; a program needn't handle non-finite values.
Results may differ from the reference program's by a relative error of at most 0.0029.
Values sent between devices are 32-bit elements; how exact they have to be, the bound alone decides.
A program may use at most 64 MiB of HBM per device.

```python
import math
import jax
import jax.numpy as jnp
from jax import lax

FACE_DEV = 256
OBS_GROUP = 256
WINDOW_STEPS = 32
SLOT_CAP = 2
LIST_LEN = 8
TOTAL_FACES = 8192
OBSERVERS = 1024
SAMPLES = 256
DEVICES = 32


def unit_vectors(key, count):
    first, second = jax.random.split(key)
    height = jax.random.uniform(first, (count,), jnp.float32, -1.0, 1.0)
    azimuth = jax.random.uniform(second, (count,), jnp.float32, -math.pi, math.pi)
    radius = jnp.sqrt(jnp.maximum(1.0 - height * height, 0.0))
    return (radius * jnp.cos(azimuth), radius * jnp.sin(azimuth), height)


def draw_normal(key, part):
    east, north, upward = unit_vectors(jax.random.fold_in(key, 11), TOTAL_FACES)
    return jnp.stack([east, north, upward], axis=0).astype(jnp.float32)


def draw_direction(key, part):
    devices = TOTAL_FACES // FACE_DEV
    east, north, upward = unit_vectors(jax.random.fold_in(key, 12), devices * LIST_LEN)
    return jnp.stack([east, north, upward], axis=-1).reshape(devices, LIST_LEN, 3).astype(jnp.float32)


def draw_bin_index(key, part):
    devices = TOTAL_FACES // FACE_DEV
    n_blocks = SAMPLES // WINDOW_STEPS

    def one_row(row_key):
        order_key, block_key = jax.random.split(row_key)
        order = jax.random.permutation(order_key, LIST_LEN)
        blocks = jax.random.permutation(block_key, n_blocks)
        return blocks[order // SLOT_CAP].astype(jnp.int32)
    return jax.vmap(one_row)(jax.random.split(jax.random.fold_in(key, 13), devices))


def draw_item_count(key, part):
    devices = TOTAL_FACES // FACE_DEV
    first, second, third = jax.random.split(jax.random.fold_in(key, 14), 3)
    base = jax.random.randint(first, (devices,), LIST_LEN // 2, LIST_LEN + 1)
    full = jax.random.randint(second, (devices,), 0, 8) == 0
    chosen = jax.random.randint(third, (), 0, devices)
    forced = jnp.arange(devices) == chosen
    return jnp.where(full | forced, LIST_LEN, jnp.minimum(base, LIST_LEN)).astype(jnp.int32)


def plant(array, rng, low, top_value):
    longest = array.shape.index(max(array.shape))
    spots = []
    for shift in (0, 1):
        where = [jax.random.randint(jax.random.fold_in(rng, axis), (), 0, length) for axis, length in enumerate(array.shape)]
        where[longest] = (where[longest] + shift) % array.shape[longest]
        spots.append(tuple(where))
    return array.at[spots[0]].set(low).at[spots[1]].set(top_value)


def steps_of(key, shape, cuts, smallest, high):
    level, own = 1.0, jax.random.fold_in(key, 6)
    for axis_at, parts in cuts:
        draws = jnp.exp(jax.random.uniform(jax.random.fold_in(own, axis_at), (parts,), jnp.float32, smallest / len(cuts), high / len(cuts)))
        level = level * jnp.repeat(draws, shape[axis_at] // parts).reshape([-1 if axis == axis_at else 1 for axis in range(len(shape))])
    return level


def bell_draw(own_key, extent, width, bound, cuts=(), kind=jnp.bfloat16):
    loudness = steps_of(own_key, extent, cuts, -0.22, 0.18) if cuts else 1.0
    result = jax.random.normal(own_key, extent, jnp.float32) * width * loudness
    return jnp.minimum(jnp.maximum(result, -bound), bound).astype(kind)


def setup_inputs(seed: int = 0) -> dict:
    splits = jax.random.split(jax.random.key(seed), 10)
    density = jnp.clip(0.6 + 0.79999995 * jax.random.uniform(splits[0], (WINDOW_STEPS + 2, TOTAL_FACES), jnp.float32) ** steps_of(splits[0], (WINDOW_STEPS + 2, TOTAL_FACES), ((1, 32),), -0.2, 0.2), 0.6, 1.4)
    velocity = bell_draw(splits[1], (3, WINDOW_STEPS + 2, TOTAL_FACES), 1.0, 6.0, ((2, 32),), jnp.float32)
    pressure = bell_draw(splits[2], (WINDOW_STEPS + 2, TOTAL_FACES), 1.0, 6.0, ((1, 32),), jnp.float32)
    normal = draw_normal(jax.random.fold_in(splits[9], 71), 0)
    direction = draw_direction(jax.random.fold_in(splits[9], 71), 0)
    weights = bell_draw(splits[5], (DEVICES, LIST_LEN, 3 * FACE_DEV, OBS_GROUP), (3 * FACE_DEV) ** -0.5, 0.21875, ((0, 32),))
    bin_index = draw_bin_index(jax.random.fold_in(splits[9], 71), 0)
    group_index = plant(jax.random.randint(splits[7], (DEVICES, LIST_LEN), 0, OBSERVERS // OBS_GROUP), jax.random.fold_in(splits[7], 1), 0, (OBSERVERS // OBS_GROUP) - 1).astype(jnp.int32)
    item_count = draw_item_count(jax.random.fold_in(splits[9], 71), 0)
    return dict(density=density, velocity=velocity, pressure=pressure, normal=normal, direction=direction, weights=weights, bin_index=bin_index, group_index=group_index, item_count=item_count)


def face_terms(dens, veloc, press, norms):
    normal_speed = veloc[0] * norms[0][None] + veloc[1] * norms[1][None] + veloc[2] * norms[2][None]
    flux = dens * normal_speed
    load_first = press * norms[0][None] + dens * veloc[0] * normal_speed
    load_second = press * norms[1][None] + dens * veloc[1] * normal_speed
    load_third = press * norms[2][None] + dens * veloc[2] * normal_speed
    thick = 0.5 * (flux[2:] - flux[:-2])
    return thick, load_first, load_second, load_third


def item_source(thick, load_first, load_second, load_third, heading):
    radial = heading[0] * load_first + heading[1] * load_second + heading[2] * load_third
    rate = 0.5 * (radial[2:] - radial[:-2])
    return jnp.concatenate([thick, rate, radial[1:-1]], axis=1).astype(jnp.bfloat16)


def reference(density, velocity, pressure, normal, direction, weights, bin_index, group_index, item_count):
    n_devices = weights.shape[0]
    per_device = density.shape[1] // n_devices
    rows = density.shape[0]
    dens_dev = density.reshape(rows, n_devices, per_device).transpose(1, 0, 2)
    press_dev = pressure.reshape(rows, n_devices, per_device).transpose(1, 0, 2)
    veloc_dev = velocity.reshape(3, rows, n_devices, per_device).transpose(2, 0, 1, 3)
    norms_dev = normal.reshape(3, n_devices, per_device).transpose(1, 0, 2)
    n_blocks = SAMPLES // WINDOW_STEPS
    n_groups = OBSERVERS // OBS_GROUP
    start = jnp.zeros((n_blocks, n_groups, WINDOW_STEPS, OBS_GROUP), jnp.float32)

    def device_step(signal, inputs):
        dens, veloc, press, norms, headings, matrices, blocks_of, groups_of, live_count = inputs
        thick, load_first, load_second, load_third = face_terms(dens, veloc, press, norms)
        for listed in range(LIST_LEN):
            source = item_source(thick, load_first, load_second, load_third, headings[listed])
            block = jnp.dot(source, matrices[listed], preferred_element_type=jnp.float32)
            switch = (listed < live_count).astype(jnp.float32)
            signal = signal.at[blocks_of[listed], groups_of[listed]].add(block * switch)
        return signal, None

    signal, _ = lax.scan(device_step, start, (dens_dev, veloc_dev, press_dev, norms_dev, direction, weights, bin_index, group_index, item_count))
    return signal.transpose(0, 2, 1, 3).reshape(SAMPLES, OBSERVERS)
```

```python
import functools

import jax
import jax.numpy as jnp
from jax import lax
from jax.experimental import pallas as pl
from jax.experimental.pallas import tpu as pltpu
from jax.sharding import PartitionSpec as P

SLOT_CAP = 2
MESH = pl.DeviceIdType.MESH


def loop(first, last, body):
    if last - first <= 8:
        for at in range(first, last):
            body(at)
    else:
        lax.fori_loop(first, last, lambda at, _: (body(at), _)[1], 0)


def kernel(
    n_obs, n_face, chunks,
    direction, bin_index, group_index, item_count,
    density, velocity, pressure, normal, weights,
    out,
    dens, veloc, press, norms, matrices, thick, rate_of, load_of, blocks,
    outgoing, arrived, labels_out, labels_in, grouped, owned,
    in_sem, weight_sem, label_send, label_recv, send_sem, recv_sem, send_two, recv_two,
):
    my_obs, my_face = lax.axis_index("obs"), lax.axis_index("face")
    list_total = matrices.shape[0]
    steps, width = thick.shape
    part = width // chunks

    loads = [
        pltpu.make_async_copy(density, dens, in_sem.at[0]),
        pltpu.make_async_copy(velocity, veloc, in_sem.at[1]),
        pltpu.make_async_copy(pressure, press, in_sem.at[2]),
        pltpu.make_async_copy(normal, norms, in_sem.at[3]),
    ]
    for copy in loads:
        copy.start()

    def weight_copy(listed):
        return pltpu.make_async_copy(
            weights.at[0, listed], matrices.at[listed], weight_sem.at[listed]
        )

    loop(0, list_total, lambda listed: weight_copy(listed).start())

    barrier = pltpu.get_barrier_semaphore()

    def greet_face(shift):
        peer = lax.rem(my_face + shift, n_face)
        pl.semaphore_signal(barrier, inc=1, device_id=(my_obs, peer), device_id_type=MESH)

    def greet_obs(shift):
        peer = lax.rem(my_obs + shift, n_obs)
        pl.semaphore_signal(barrier, inc=1, device_id=(peer, my_face), device_id_type=MESH)

    loop(1, n_face, greet_face)
    loop(1, n_obs, greet_obs)

    live_count = item_count[0]

    def slots_of(block):
        last = jnp.int32(-1)
        first = jnp.int32(-1)
        for listed in range(list_total):
            match = (bin_index[0, listed] == block) & (listed < live_count)
            last = jnp.where(match, listed, last)
        for listed in reversed(range(list_total)):
            match = (bin_index[0, listed] == block) & (listed < live_count)
            first = jnp.where(match, listed, first)
        return first, last

    upper = lax.broadcasted_iota(jnp.int32, labels_out.shape[1:], 0) < 4

    def fill_labels(block):
        first, last = slots_of(block)
        label_first = group_index[0, jnp.maximum(first, 0)]
        label_last = group_index[0, jnp.maximum(last, 0)]
        return jnp.where(upper, label_first, label_last)

    def label_copy(shift):
        peer = lax.rem(my_face + shift, n_face)
        return pltpu.make_async_remote_copy(
            src_ref=labels_out.at[peer],
            dst_ref=labels_in.at[my_face],
            send_sem=label_send.at[shift - 1],
            recv_sem=label_recv.at[shift - 1],
            device_id=(my_obs, peer),
            device_id_type=MESH,
        )

    def set_label(shift):
        peer = lax.rem(my_face + shift, n_face)
        labels_out[peer] = fill_labels(peer)

    loop(1, n_face, set_label)
    pl.semaphore_wait(barrier, n_face + n_obs - 2)
    loop(1, n_face, lambda shift: label_copy(shift).start())

    for copy in loads:
        copy.wait()
    n0, n1, n2 = norms[0:1], norms[1:2], norms[2:3]
    v0, v1, v2 = veloc[0], veloc[1], veloc[2]
    density_now, pressure_now = dens[...], press[...]
    normal_speed = v0 * n0 + v1 * n1 + v2 * n2
    flux = density_now * normal_speed
    thick[...] = (0.5 * (flux[2:] - flux[:-2])).astype(jnp.bfloat16)
    for c, (n, v) in enumerate(((n0, v0), (n1, v1), (n2, v2))):
        load = pressure_now * n + density_now * v * normal_speed
        rate_of[c] = 0.5 * (load[2:] - load[:-2])
        load_of[c] = load[1:-1]

    def compute(listed):
        h0, h1, h2 = (direction[0, listed, c] for c in range(3))
        rate = h0 * rate_of[0] + h1 * rate_of[1] + h2 * rate_of[2]
        radial = h0 * load_of[0] + h1 * load_of[1] + h2 * load_of[2]
        source = jnp.concatenate(
            [thick[...], rate.astype(jnp.bfloat16), radial.astype(jnp.bfloat16)], axis=1
        )
        weight_copy(listed).wait()
        blocks[listed] = jnp.dot(source, matrices[listed], preferred_element_type=jnp.float32)

    loop(0, list_total, compute)

    def data_copy(chunk, shift):
        peer = lax.rem(my_face + shift, n_face)
        return pltpu.make_async_remote_copy(
            src_ref=outgoing.at[chunk, peer],
            dst_ref=arrived.at[chunk, my_face],
            send_sem=send_sem.at[chunk, shift - 1],
            recv_sem=recv_sem.at[chunk, shift - 1],
            device_id=(my_obs, peer),
            device_id_type=MESH,
        )

    def route(chunk, block):
        first, last = slots_of(block)
        columns = pl.ds(chunk * part, part)
        early = blocks[jnp.maximum(first, 0), :, columns]
        late = blocks[jnp.maximum(last, 0), :, columns]
        return jnp.where(last >= 0, early, 0.0), jnp.where(last > first, late, 0.0)

    for chunk in range(chunks):
        def send(shift):
            peer = lax.rem(my_face + shift, n_face)
            early, late = route(chunk, peer)
            outgoing[chunk, peer, :steps] = early
            outgoing[chunk, peer, steps:] = late
            data_copy(chunk, shift).start()

        loop(1, n_face, send)

    def selected(early, late, label_first, label_last):
        return [
            jnp.where(label_first == group, early, 0.0) + jnp.where(label_last == group, late, 0.0)
            for group in range(n_obs)
        ]

    def obs_copy(chunk, shift):
        peer = lax.rem(my_obs + shift, n_obs)
        return pltpu.make_async_remote_copy(
            src_ref=grouped.at[chunk, peer],
            dst_ref=owned.at[chunk, my_obs],
            send_sem=send_two.at[chunk, shift - 1],
            recv_sem=recv_two.at[chunk, shift - 1],
            device_id=(peer, my_face),
            device_id_type=MESH,
        )

    own_labels = fill_labels(my_face)
    for chunk in range(chunks):
        early, late = route(chunk, my_face)
        sums = tuple(selected(early, late, own_labels[0:1], own_labels[4:5]))

        def collect(shift, sums, chunk=chunk):
            source = lax.rem(my_face + n_face - shift, n_face)
            if chunk == 0:
                label_copy(shift).wait_recv()
            data_copy(chunk, shift).wait_recv()
            labels = labels_in[source]
            both = arrived[chunk, source]
            terms = selected(both[:steps], both[steps:], labels[0:1], labels[4:5])
            return tuple(a + b for a, b in zip(sums, terms))

        if n_face <= 8:
            for shift in range(1, n_face):
                sums = collect(shift, sums)
        else:
            sums = lax.fori_loop(1, n_face, collect, sums)
        for group in range(n_obs):
            grouped[chunk, group] = sums[group]
        loop(1, n_obs, lambda shift: obs_copy(chunk, shift).start())

    for chunk in range(chunks):
        total = grouped[chunk, my_obs]
        for shift in range(1, n_obs):
            source = lax.rem(my_obs + n_obs - shift, n_obs)
            obs_copy(chunk, shift).wait_recv()
            total = total + owned[chunk, source]
        out[:, chunk * part:(chunk + 1) * part] = total

    for chunk in range(chunks):
        loop(1, n_face, lambda shift: data_copy(chunk, shift).wait_send())
        loop(1, n_obs, lambda shift: obs_copy(chunk, shift).wait_send())
    loop(1, n_face, lambda shift: label_copy(shift).wait_send())


def local(
    density, velocity, pressure, normal, direction, weights, bin_index, group_index, item_count
):
    n_face, n_obs = lax.axis_size("face"), lax.axis_size("obs")
    list_total, depth, width = weights.shape[1:]
    rows, faces = density.shape
    steps = rows - 2
    chunks = max(1, width // 128)
    part = width // chunks
    smem = pl.BlockSpec(memory_space=pltpu.SMEM)
    anywhere = pl.BlockSpec(memory_space=pl.ANY)
    f32 = jnp.float32
    return pl.pallas_call(
        functools.partial(kernel, n_obs, n_face, chunks),
        out_shape=jax.ShapeDtypeStruct((steps, width), f32),
        in_specs=[smem] * 4 + [anywhere] * 5,
        out_specs=pl.BlockSpec(memory_space=pltpu.VMEM),
        scratch_shapes=[
            pltpu.VMEM((rows, faces), f32),
            pltpu.VMEM((3, rows, faces), f32),
            pltpu.VMEM((rows, faces), f32),
            pltpu.VMEM((3, faces), f32),
            pltpu.VMEM((list_total, depth, width), jnp.bfloat16),
            pltpu.VMEM((steps, faces), jnp.bfloat16),
            pltpu.VMEM((3, steps, faces), f32),
            pltpu.VMEM((3, steps, faces), f32),
            pltpu.VMEM((list_total, steps, width), f32),
            pltpu.VMEM((chunks, n_face, SLOT_CAP * steps, part), f32),
            pltpu.VMEM((chunks, n_face, SLOT_CAP * steps, part), f32),
            pltpu.VMEM((n_face, 8, 128), jnp.int32),
            pltpu.VMEM((n_face, 8, 128), jnp.int32),
            pltpu.VMEM((chunks, n_obs, steps, part), f32),
            pltpu.VMEM((chunks, n_obs, steps, part), f32),
            pltpu.SemaphoreType.DMA((4,)),
            pltpu.SemaphoreType.DMA((list_total,)),
            pltpu.SemaphoreType.DMA((n_face - 1,)),
            pltpu.SemaphoreType.DMA((n_face - 1,)),
            pltpu.SemaphoreType.DMA((chunks, n_face - 1)),
            pltpu.SemaphoreType.DMA((chunks, n_face - 1)),
            pltpu.SemaphoreType.DMA((chunks, n_obs - 1)),
            pltpu.SemaphoreType.DMA((chunks, n_obs - 1)),
        ],
        compiler_params=pltpu.CompilerParams(
            collective_id=0, has_side_effects=True
        ),
    )(
        direction, bin_index, group_index, item_count,
        density, velocity, pressure, normal, weights,
    )


def solution(mesh):
    placed = (
        P(None, ("obs", "face")),
        P(None, None, ("obs", "face")),
        P(None, ("obs", "face")),
        P(None, ("obs", "face")),
        P(("obs", "face"), None, None),
        P(("obs", "face"), None, None, None),
        P(("obs", "face"), None),
        P(("obs", "face"), None),
        P(("obs", "face")),
    )
    return jax.shard_map(
        local, mesh=mesh, in_specs=placed, out_specs=P("face", "obs"), check_vma=False
    )
```

```python
import functools

import jax
import jax.numpy as jnp
from jax import lax
from jax.experimental import pallas as pl
from jax.experimental.pallas import tpu as pltpu
from jax.sharding import PartitionSpec as P

SLOT_CAP = 2
MESH = pl.DeviceIdType.MESH


def loop(first, last, body):
    if last - first <= 8:
        for at in range(first, last):
            body(at)
    else:
        lax.fori_loop(first, last, lambda at, _: (body(at), _)[1], 0)


def kernel(
    n_obs, n_face, chunks,
    direction, bin_index, group_index, item_count,
    density, velocity, pressure, normal, weights,
    out,
    dens, veloc, press, norms, matrices, thick, rate_of, load_of, sources, blocks,
    outgoing, arrived, labels_out, labels_in, grouped, owned,
    in_sem, weight_sem, label_send, label_recv, send_sem, recv_sem, send_two, recv_two,
):
    my_obs, my_face = lax.axis_index("obs"), lax.axis_index("face")
    list_total = matrices.shape[1]
    steps, width = thick.shape
    part = width // chunks

    loads = [
        pltpu.make_async_copy(density, dens, in_sem.at[0]),
        pltpu.make_async_copy(velocity, veloc, in_sem.at[1]),
        pltpu.make_async_copy(pressure, press, in_sem.at[2]),
        pltpu.make_async_copy(normal, norms, in_sem.at[3]),
    ]
    for copy in loads:
        copy.start()

    def weight_copy(chunk, listed):
        return pltpu.make_async_copy(
            weights.at[0, listed, :, pl.ds(chunk * part, part)],
            matrices.at[chunk, listed],
            weight_sem.at[chunk, listed],
        )

    for chunk in range(chunks):
        loop(0, list_total, lambda listed: weight_copy(chunk, listed).start())

    barrier = pltpu.get_barrier_semaphore()

    def greet_face(shift):
        peer = lax.rem(my_face + shift, n_face)
        pl.semaphore_signal(barrier, inc=1, device_id=(my_obs, peer), device_id_type=MESH)

    def greet_obs(shift):
        peer = lax.rem(my_obs + shift, n_obs)
        pl.semaphore_signal(barrier, inc=1, device_id=(peer, my_face), device_id_type=MESH)

    loop(1, n_face, greet_face)
    loop(1, n_obs, greet_obs)

    live_count = item_count[0]

    def slots_of(block):
        last = jnp.int32(-1)
        first = jnp.int32(-1)
        for listed in range(list_total):
            match = (bin_index[0, listed] == block) & (listed < live_count)
            last = jnp.where(match, listed, last)
        for listed in reversed(range(list_total)):
            match = (bin_index[0, listed] == block) & (listed < live_count)
            first = jnp.where(match, listed, first)
        return first, last

    upper = lax.broadcasted_iota(jnp.int32, labels_out.shape[1:], 0) < 4

    def fill_labels(block):
        first, last = slots_of(block)
        label_first = group_index[0, jnp.maximum(first, 0)]
        label_last = group_index[0, jnp.maximum(last, 0)]
        return jnp.where(upper, label_first, label_last)

    def label_copy(shift):
        peer = lax.rem(my_face + shift, n_face)
        return pltpu.make_async_remote_copy(
            src_ref=labels_out.at[peer],
            dst_ref=labels_in.at[my_face],
            send_sem=label_send.at[shift - 1],
            recv_sem=label_recv.at[shift - 1],
            device_id=(my_obs, peer),
            device_id_type=MESH,
        )

    def set_label(shift):
        peer = lax.rem(my_face + shift, n_face)
        labels_out[peer] = fill_labels(peer)

    loop(1, n_face, set_label)

    for copy in loads:
        copy.wait()
    n0, n1, n2 = norms[0:1], norms[1:2], norms[2:3]
    v0, v1, v2 = veloc[0], veloc[1], veloc[2]
    density_now, pressure_now = dens[...], press[...]
    normal_speed = v0 * n0 + v1 * n1 + v2 * n2
    flux = density_now * normal_speed
    thick[...] = (0.5 * (flux[2:] - flux[:-2])).astype(jnp.bfloat16)
    for c, (n, v) in enumerate(((n0, v0), (n1, v1), (n2, v2))):
        load = pressure_now * n + density_now * v * normal_speed
        rate_of[c] = 0.5 * (load[2:] - load[:-2])
        load_of[c] = load[1:-1]

    def prepare(listed):
        h0, h1, h2 = (direction[c, 0, listed] for c in range(3))
        rate = h0 * rate_of[0] + h1 * rate_of[1] + h2 * rate_of[2]
        radial = h0 * load_of[0] + h1 * load_of[1] + h2 * load_of[2]
        sources[listed] = jnp.concatenate(
            [thick[...], rate.astype(jnp.bfloat16), radial.astype(jnp.bfloat16)], axis=1
        )

    loop(0, list_total, prepare)
    pl.semaphore_wait(barrier, n_face + n_obs - 2)
    loop(1, n_face, lambda shift: label_copy(shift).start())

    def compute(chunk, listed):
        weight_copy(chunk, listed).wait()
        blocks[chunk, listed] = jnp.dot(
            sources[listed], matrices[chunk, listed], preferred_element_type=jnp.float32
        )

    def data_copy(chunk, shift):
        peer = lax.rem(my_face + shift, n_face)
        return pltpu.make_async_remote_copy(
            src_ref=outgoing.at[chunk, peer],
            dst_ref=arrived.at[chunk, my_face],
            send_sem=send_sem.at[chunk, shift - 1],
            recv_sem=recv_sem.at[chunk, shift - 1],
            device_id=(my_obs, peer),
            device_id_type=MESH,
        )

    def route(chunk, block):
        first, last = slots_of(block)
        early = blocks[chunk, jnp.maximum(first, 0)]
        late = blocks[chunk, jnp.maximum(last, 0)]
        return jnp.where(last >= 0, early, 0.0), jnp.where(last > first, late, 0.0)

    for chunk in range(chunks):
        loop(0, list_total, functools.partial(compute, chunk))

        def send(shift):
            peer = lax.rem(my_face + shift, n_face)
            early, late = route(chunk, peer)
            outgoing[chunk, peer, :steps] = early
            outgoing[chunk, peer, steps:] = late
            data_copy(chunk, shift).start()

        loop(1, n_face, send)

    def selected(early, late, label_first, label_last):
        return [
            jnp.where(label_first == group, early, 0.0) + jnp.where(label_last == group, late, 0.0)
            for group in range(n_obs)
        ]

    def obs_copy(chunk, shift):
        peer = lax.rem(my_obs + shift, n_obs)
        return pltpu.make_async_remote_copy(
            src_ref=grouped.at[chunk, peer],
            dst_ref=owned.at[chunk, my_obs],
            send_sem=send_two.at[chunk, shift - 1],
            recv_sem=recv_two.at[chunk, shift - 1],
            device_id=(peer, my_face),
            device_id_type=MESH,
        )

    own_labels = fill_labels(my_face)
    for chunk in range(chunks):
        early, late = route(chunk, my_face)
        sums = tuple(selected(early, late, own_labels[0:1], own_labels[4:5]))

        def collect(shift, sums, chunk=chunk):
            source = lax.rem(my_face + n_face - shift, n_face)
            if chunk == 0:
                label_copy(shift).wait_recv()
            data_copy(chunk, shift).wait_recv()
            labels = labels_in[source]
            both = arrived[chunk, source]
            terms = selected(both[:steps], both[steps:], labels[0:1], labels[4:5])
            return tuple(a + b for a, b in zip(sums, terms))

        if n_face <= 8:
            for shift in range(1, n_face):
                sums = collect(shift, sums)
        else:
            sums = lax.fori_loop(1, n_face, collect, sums)
        for group in range(n_obs):
            grouped[chunk, group] = sums[group]
        loop(1, n_obs, lambda shift: obs_copy(chunk, shift).start())

    for chunk in range(chunks):
        total = grouped[chunk, my_obs]
        for shift in range(1, n_obs):
            source = lax.rem(my_obs + n_obs - shift, n_obs)
            obs_copy(chunk, shift).wait_recv()
            total = total + owned[chunk, source]
        out[:, chunk * part:(chunk + 1) * part] = total

    for chunk in range(chunks):
        loop(1, n_face, lambda shift: data_copy(chunk, shift).wait_send())
        loop(1, n_obs, lambda shift: obs_copy(chunk, shift).wait_send())
    loop(1, n_face, lambda shift: label_copy(shift).wait_send())


def local(
    density, velocity, pressure, normal, direction, weights, bin_index, group_index, item_count
):
    n_face, n_obs = lax.axis_size("face"), lax.axis_size("obs")
    list_total, depth, width = weights.shape[1:]
    rows, faces = density.shape
    steps = rows - 2
    chunks = max(1, width // 128)
    part = width // chunks
    smem = pl.BlockSpec(memory_space=pltpu.SMEM)
    anywhere = pl.BlockSpec(memory_space=pl.ANY)
    f32 = jnp.float32
    return pl.pallas_call(
        functools.partial(kernel, n_obs, n_face, chunks),
        out_shape=pltpu.VMEM((steps, width), f32),
        in_specs=[smem] * 4 + [anywhere] * 5,
        out_specs=pl.BlockSpec(memory_space=pltpu.VMEM),
        scratch_shapes=[
            pltpu.VMEM((rows, faces), f32),
            pltpu.VMEM((3, rows, faces), f32),
            pltpu.VMEM((rows, faces), f32),
            pltpu.VMEM((3, faces), f32),
            pltpu.VMEM((chunks, list_total, depth, part), jnp.bfloat16),
            pltpu.VMEM((steps, faces), jnp.bfloat16),
            pltpu.VMEM((3, steps, faces), f32),
            pltpu.VMEM((3, steps, faces), f32),
            pltpu.VMEM((list_total, steps, depth), jnp.bfloat16),
            pltpu.VMEM((chunks, list_total, steps, part), f32),
            pltpu.VMEM((chunks, n_face, SLOT_CAP * steps, part), f32),
            pltpu.VMEM((chunks, n_face, SLOT_CAP * steps, part), f32),
            pltpu.VMEM((n_face, 8, part), jnp.int32),
            pltpu.VMEM((n_face, 8, part), jnp.int32),
            pltpu.VMEM((chunks, n_obs, steps, part), f32),
            pltpu.VMEM((chunks, n_obs, steps, part), f32),
            pltpu.SemaphoreType.DMA((4,)),
            pltpu.SemaphoreType.DMA((chunks, list_total)),
            pltpu.SemaphoreType.DMA((n_face - 1,)),
            pltpu.SemaphoreType.DMA((n_face - 1,)),
            pltpu.SemaphoreType.DMA((chunks, n_face - 1)),
            pltpu.SemaphoreType.DMA((chunks, n_face - 1)),
            pltpu.SemaphoreType.DMA((chunks, n_obs - 1)),
            pltpu.SemaphoreType.DMA((chunks, n_obs - 1)),
        ],
        compiler_params=pltpu.CompilerParams(
            collective_id=0, has_side_effects=True
        ),
    )(
        jnp.transpose(direction, (2, 0, 1)), bin_index, group_index, item_count,
        density, velocity, pressure, normal, weights,
    )


def solution(mesh):
    placed = (
        P(None, ("obs", "face")),
        P(None, None, ("obs", "face")),
        P(None, ("obs", "face")),
        P(None, ("obs", "face")),
        P(("obs", "face"), None, None),
        P(("obs", "face"), None, None, None),
        P(("obs", "face"), None),
        P(("obs", "face"), None),
        P(("obs", "face")),
    )
    return jax.shard_map(
        local, mesh=mesh, in_specs=placed, out_specs=P("face", "obs"), check_vma=False
    )
```

```python
import functools

import jax
import jax.numpy as jnp
from jax import lax
from jax.experimental import pallas as pl
from jax.experimental.pallas import tpu as pltpu
from jax.sharding import PartitionSpec as P

SLOT_CAP = 2
MESH = pl.DeviceIdType.MESH


def loop(first, last, body):
    if last - first <= 8:
        for at in range(first, last):
            body(at)
    else:
        lax.fori_loop(first, last, lambda at, _: (body(at), _)[1], 0)


def kernel(
    n_obs, n_face, chunks,
    direction, bin_index, group_index, item_count,
    density, velocity, pressure, normal, weights,
    out,
    dens, veloc, press, norms, matrices, thick, rate_of, load_of, sources, blocks,
    outgoing, arrived, labels_out, labels_in, grouped, owned,
    in_sem, weight_sem, label_send, label_recv, send_sem, recv_sem, send_two, recv_two,
):
    my_obs, my_face = lax.axis_index("obs"), lax.axis_index("face")
    list_total = matrices.shape[1]
    steps, width = thick.shape
    part = width // chunks

    loads = [
        pltpu.make_async_copy(density, dens, in_sem.at[0]),
        pltpu.make_async_copy(velocity, veloc, in_sem.at[1]),
        pltpu.make_async_copy(pressure, press, in_sem.at[2]),
        pltpu.make_async_copy(normal, norms, in_sem.at[3]),
    ]
    for copy in loads:
        copy.start()

    def weight_copy(chunk, listed):
        return pltpu.make_async_copy(
            weights.at[0, listed, :, pl.ds(chunk * part, part)],
            matrices.at[chunk, listed],
            weight_sem.at[chunk, listed],
        )

    for chunk in range(chunks):
        loop(0, list_total, lambda listed: weight_copy(chunk, listed).start())

    barrier = pltpu.get_barrier_semaphore()

    def greet_face(shift):
        peer = lax.rem(my_face + shift, n_face)
        pl.semaphore_signal(barrier, inc=1, device_id=(my_obs, peer), device_id_type=MESH)

    def greet_obs(shift):
        peer = lax.rem(my_obs + shift, n_obs)
        pl.semaphore_signal(barrier, inc=1, device_id=(peer, my_face), device_id_type=MESH)

    loop(1, n_face, greet_face)
    loop(1, n_obs, greet_obs)

    live_count = item_count[0]

    def slots_of(block):
        last = jnp.int32(-1)
        first = jnp.int32(-1)
        for listed in range(list_total):
            match = (bin_index[0, listed] == block) & (listed < live_count)
            last = jnp.where(match, listed, last)
        for listed in reversed(range(list_total)):
            match = (bin_index[0, listed] == block) & (listed < live_count)
            first = jnp.where(match, listed, first)
        return first, last

    upper = lax.broadcasted_iota(jnp.int32, labels_out.shape[1:], 0) < 4

    def fill_labels(block):
        first, last = slots_of(block)
        label_first = group_index[0, jnp.maximum(first, 0)]
        label_last = group_index[0, jnp.maximum(last, 0)]
        return jnp.where(upper, label_first, label_last)

    def label_copy(shift):
        peer = lax.rem(my_face + shift, n_face)
        return pltpu.make_async_remote_copy(
            src_ref=labels_out.at[peer],
            dst_ref=labels_in.at[my_face],
            send_sem=label_send.at[shift - 1],
            recv_sem=label_recv.at[shift - 1],
            device_id=(my_obs, peer),
            device_id_type=MESH,
        )

    def set_label(shift):
        peer = lax.rem(my_face + shift, n_face)
        labels_out[peer] = fill_labels(peer)

    loop(1, n_face, set_label)

    for copy in loads:
        copy.wait()
    n0, n1, n2 = norms[0:1], norms[1:2], norms[2:3]
    v0, v1, v2 = veloc[0], veloc[1], veloc[2]
    density_now, pressure_now = dens[...], press[...]
    normal_speed = v0 * n0 + v1 * n1 + v2 * n2
    flux = density_now * normal_speed
    thick[...] = (0.5 * (flux[2:] - flux[:-2])).astype(jnp.bfloat16)
    for c, (n, v) in enumerate(((n0, v0), (n1, v1), (n2, v2))):
        load = pressure_now * n + density_now * v * normal_speed
        rate_of[c] = 0.5 * (load[2:] - load[:-2])
        load_of[c] = load[1:-1]

    def prepare(listed):
        h0, h1, h2 = (direction[c, 0, listed] for c in range(3))
        rate = h0 * rate_of[0] + h1 * rate_of[1] + h2 * rate_of[2]
        radial = h0 * load_of[0] + h1 * load_of[1] + h2 * load_of[2]
        sources[listed] = jnp.concatenate(
            [thick[...], rate.astype(jnp.bfloat16), radial.astype(jnp.bfloat16)], axis=1
        )

    loop(0, list_total, prepare)
    pl.semaphore_wait(barrier, n_face + n_obs - 2)
    loop(1, n_face, lambda shift: label_copy(shift).start())

    batch = 8 if list_total % 8 == 0 else 1

    def compute(chunk, at):
        members = [at * batch + offset for offset in range(batch)]
        for listed in members:
            weight_copy(chunk, listed).wait()
        products = [
            jnp.dot(sources[listed], matrices[chunk, listed], preferred_element_type=jnp.float32)
            for listed in members
        ]
        for listed, product in zip(members, products):
            blocks[chunk, listed] = product

    def data_copy(chunk, shift):
        peer = lax.rem(my_face + shift, n_face)
        return pltpu.make_async_remote_copy(
            src_ref=outgoing.at[chunk, peer],
            dst_ref=arrived.at[chunk, my_face],
            send_sem=send_sem.at[chunk, shift - 1],
            recv_sem=recv_sem.at[chunk, shift - 1],
            device_id=(my_obs, peer),
            device_id_type=MESH,
        )

    def route(chunk, block):
        first, last = slots_of(block)
        early = blocks[chunk, jnp.maximum(first, 0)]
        late = blocks[chunk, jnp.maximum(last, 0)]
        return jnp.where(last >= 0, early, 0.0), jnp.where(last > first, late, 0.0)

    for chunk in range(chunks):
        loop(0, list_total // batch, functools.partial(compute, chunk))

        def send(shift):
            peer = lax.rem(my_face + shift, n_face)
            early, late = route(chunk, peer)
            outgoing[chunk, peer, :steps] = early
            outgoing[chunk, peer, steps:] = late
            data_copy(chunk, shift).start()

        loop(1, n_face, send)

    def selected(early, late, label_first, label_last):
        return [
            jnp.where(label_first == group, early, 0.0) + jnp.where(label_last == group, late, 0.0)
            for group in range(n_obs)
        ]

    def obs_copy(chunk, shift):
        peer = lax.rem(my_obs + shift, n_obs)
        return pltpu.make_async_remote_copy(
            src_ref=grouped.at[chunk, peer],
            dst_ref=owned.at[chunk, my_obs],
            send_sem=send_two.at[chunk, shift - 1],
            recv_sem=recv_two.at[chunk, shift - 1],
            device_id=(peer, my_face),
            device_id_type=MESH,
        )

    own_labels = fill_labels(my_face)
    for chunk in range(chunks):
        early, late = route(chunk, my_face)
        sums = tuple(selected(early, late, own_labels[0:1], own_labels[4:5]))

        def collect(shift, sums, chunk=chunk):
            source = lax.rem(my_face + n_face - shift, n_face)
            if chunk == 0:
                label_copy(shift).wait_recv()
            data_copy(chunk, shift).wait_recv()
            labels = labels_in[source]
            both = arrived[chunk, source]
            terms = selected(both[:steps], both[steps:], labels[0:1], labels[4:5])
            return tuple(a + b for a, b in zip(sums, terms))

        if n_face <= 8:
            for shift in range(1, n_face):
                sums = collect(shift, sums)
        else:
            sums = lax.fori_loop(1, n_face, collect, sums)
        for group in range(n_obs):
            grouped[chunk, group] = sums[group]
        loop(1, n_obs, lambda shift: obs_copy(chunk, shift).start())

    for chunk in range(chunks):
        total = grouped[chunk, my_obs]
        for shift in range(1, n_obs):
            source = lax.rem(my_obs + n_obs - shift, n_obs)
            obs_copy(chunk, shift).wait_recv()
            total = total + owned[chunk, source]
        out[:, chunk * part:(chunk + 1) * part] = total

    for chunk in range(chunks):
        loop(1, n_face, lambda shift: data_copy(chunk, shift).wait_send())
        loop(1, n_obs, lambda shift: obs_copy(chunk, shift).wait_send())
    loop(1, n_face, lambda shift: label_copy(shift).wait_send())


def local(
    density, velocity, pressure, normal, direction, weights, bin_index, group_index, item_count
):
    n_face, n_obs = lax.axis_size("face"), lax.axis_size("obs")
    list_total, depth, width = weights.shape[1:]
    rows, faces = density.shape
    steps = rows - 2
    chunks = max(1, width // 128)
    part = width // chunks
    smem = pl.BlockSpec(memory_space=pltpu.SMEM)
    anywhere = pl.BlockSpec(memory_space=pl.ANY)
    f32 = jnp.float32
    return pl.pallas_call(
        functools.partial(kernel, n_obs, n_face, chunks),
        out_shape=pltpu.VMEM((steps, width), f32),
        in_specs=[smem] * 4 + [anywhere] * 5,
        out_specs=pl.BlockSpec(memory_space=pltpu.VMEM),
        scratch_shapes=[
            pltpu.VMEM((rows, faces), f32),
            pltpu.VMEM((3, rows, faces), f32),
            pltpu.VMEM((rows, faces), f32),
            pltpu.VMEM((3, faces), f32),
            pltpu.VMEM((chunks, list_total, depth, part), jnp.bfloat16),
            pltpu.VMEM((steps, faces), jnp.bfloat16),
            pltpu.VMEM((3, steps, faces), f32),
            pltpu.VMEM((3, steps, faces), f32),
            pltpu.VMEM((list_total, steps, depth), jnp.bfloat16),
            pltpu.VMEM((chunks, list_total, steps, part), f32),
            pltpu.VMEM((chunks, n_face, SLOT_CAP * steps, part), f32),
            pltpu.VMEM((chunks, n_face, SLOT_CAP * steps, part), f32),
            pltpu.VMEM((n_face, 8, part), jnp.int32),
            pltpu.VMEM((n_face, 8, part), jnp.int32),
            pltpu.VMEM((chunks, n_obs, steps, part), f32),
            pltpu.VMEM((chunks, n_obs, steps, part), f32),
            pltpu.SemaphoreType.DMA((4,)),
            pltpu.SemaphoreType.DMA((chunks, list_total)),
            pltpu.SemaphoreType.DMA((n_face - 1,)),
            pltpu.SemaphoreType.DMA((n_face - 1,)),
            pltpu.SemaphoreType.DMA((chunks, n_face - 1)),
            pltpu.SemaphoreType.DMA((chunks, n_face - 1)),
            pltpu.SemaphoreType.DMA((chunks, n_obs - 1)),
            pltpu.SemaphoreType.DMA((chunks, n_obs - 1)),
        ],
        compiler_params=pltpu.CompilerParams(
            collective_id=0, has_side_effects=True
        ),
    )(
        jnp.transpose(direction, (2, 0, 1)), bin_index, group_index, item_count,
        density, velocity, pressure, normal, weights,
    )


def solution(mesh):
    placed = (
        P(None, ("obs", "face")),
        P(None, None, ("obs", "face")),
        P(None, ("obs", "face")),
        P(None, ("obs", "face")),
        P(("obs", "face"), None, None),
        P(("obs", "face"), None, None, None),
        P(("obs", "face"), None),
        P(("obs", "face"), None),
        P(("obs", "face")),
    )
    return jax.shard_map(
        local, mesh=mesh, in_specs=placed, out_specs=P("face", "obs"), check_vma=False
    )
```
